32 devices in a mesh: grp: 8 (over y, x, core), tile: 4 (over z).
Axes of the slice: x: 2, y: 2, z: 4, core: 2. Of those that a mesh axis runs over, the one named last changes fastest.
Arguments:
- atm_flux: float32 [6, 32768], P(None, ('grp', 'tile')), may hold values from -6 to 6
- send_block: int32 [32, 4, 4], P(('grp', 'tile')), may hold values from 0 to 7
- send_count: int32 [32, 4], P(('grp', 'tile')), may hold values from 1 to 4, as said below
- recv_block: int32 [32, 4, 4], P(('grp', 'tile')), may hold values from 0 to 63
- recv_weight: bfloat16 [32, 4, 4, 128, 128], P(('grp', 'tile')), may hold values from -0.5 to 0.5
- sea_temp: float32 [256, 1024], P('grp', 'tile'), may hold values from -6 to 6
- ocean_mask: int32 [256, 1024], P('grp', 'tile'), may hold values 0 or 1
Outputs:
- heat_flux: float32 [256, 1024], P('grp', 'tile')
- stress_curl: float32 [256, 1024], P('grp', 'tile')
- atm_return: float32 [4, 32768], P(None, ('grp', 'tile'))
The draws below stay inside these ranges and needn't reach their ends.
Inputs may be any that keep to these rules, and one draw needn't show every extreme that they name: `send_count`: in every draw a quarter of the tile indices, drawn from the seed, receive exactly 4 blocks from every device of their group; every other pair carries 1 to 2 blocks.
All inputs are finite; a program needn't handle non-finite values. No bound on the sum of `ocean_mask` on one device may be relied on, other than what follows from the above.
Results may differ from the reference program's by a relative error of at most 0.0003.
Values sent between devices are 32-bit elements; how exact they have to be, the bound alone decides.
A program may use at most 64 MiB of HBM per device.

```python
import jax
import jax.numpy as jnp
from jax import lax

NF = 6
NB = 4
BLK = 128
CAP = 4
ABLK_DEV = 8
OROW = 32
OCOL = 256
OBLK = 64
NYO = 256
NXO = 1024
ACELLS = 32768
N_GRP = 8
N_TILE = 4
DEVICES = 32


def draw_send_count(key, part):
    first_key, second_key = jax.random.split(jax.random.fold_in(key, 11))
    base_count = jax.random.randint(first_key, (DEVICES, N_TILE), 1, CAP // 2 + 1)
    offset = jax.random.randint(second_key, (), 0, 4)
    column = jnp.arange(N_TILE, dtype=jnp.int32)
    busy = ((column + offset) % 4 == 0)[None, :]
    return jnp.where(busy, CAP, base_count).astype(jnp.int32)


def set_ends(drawn, key, least, high):
    longest = drawn.shape.index(max(drawn.shape))
    spots = []
    for shift in (0, 1):
        where = [jax.random.randint(jax.random.fold_in(key, axis), (), 0, length) for axis, length in enumerate(drawn.shape)]
        where[longest] = (where[longest] + shift) % drawn.shape[longest]
        spots.append(tuple(where))
    return drawn.at[spots[0]].set(least).at[spots[1]].set(high)


def shard_levels(stream_key, extent, cuts, smallest, largest):
    def one(dim, parts):
        heights = jax.random.uniform(jax.random.fold_in(jax.random.fold_in(stream_key, 6), dim), (parts,), jnp.float32, smallest / len(cuts), largest / len(cuts))
        return jnp.repeat(jnp.exp(heights), extent[dim] // parts).reshape((-1,) + (1,) * (len(extent) - dim - 1))

    loudness = one(*cuts[0])
    for cut in cuts[1:]:
        loudness = loudness * one(*cut)
    return loudness


def noise(key, extent, deviation, reach, cuts=(), kind=jnp.bfloat16):
    values = deviation * jax.random.normal(key, extent, jnp.float32)
    if cuts:
        values = values * shard_levels(key, extent, cuts, -0.22, 0.18)
    return jnp.clip(values, -reach, reach).astype(kind)


def setup_inputs(seed: int = 0) -> dict:
    key_of = jax.random.split(jax.random.key(seed), 8)
    return {
        "atm_flux": noise(key_of[0], (NF, ACELLS), 1.0, 6.0, ((1, 32),), jnp.float32),
        "send_block": set_ends(jax.random.randint(key_of[1], (DEVICES, N_TILE, CAP), 0, ABLK_DEV), jax.random.fold_in(key_of[1], 1), 0, ABLK_DEV - 1).astype(jnp.int32),
        "send_count": draw_send_count(jax.random.fold_in(key_of[7], 71), 0),
        "recv_block": set_ends(jax.random.randint(key_of[3], (DEVICES, N_TILE, CAP), 0, OBLK), jax.random.fold_in(key_of[3], 1), 0, OBLK - 1).astype(jnp.int32),
        "recv_weight": noise(key_of[4], (DEVICES, N_TILE, CAP, BLK, BLK), BLK ** -0.5, 0.5, ((0, 32),)),
        "sea_temp": noise(key_of[5], (NYO, NXO), 1.0, 6.0, ((0, 8), (1, 4)), jnp.float32),
        "ocean_mask": set_ends((jax.random.randint(key_of[6], (NYO, NXO), 0, 10) < 7).astype(jnp.int32), jax.random.fold_in(key_of[6], 1), 0, 1),
    }


precise = lax.Precision.HIGHEST

def bulk_formula(fields, surface_temp, ocean_mask):
    sea_share = ocean_mask.astype(jnp.float32)
    wind_u, wind_v, air_temp, air_vapor, short_down, long_down = [fields[k] for k in range(6)]
    wind_speed = jnp.sqrt(wind_u * wind_u + wind_v * wind_v + 0.5)
    stress_x = 0.8 * wind_speed * wind_u * sea_share
    stress_y = 0.8 * wind_speed * wind_v * sea_share
    sensible = 0.6 * wind_speed * (surface_temp - air_temp)
    latent = 0.7 * wind_speed * (jnp.exp(0.3 * surface_temp) - air_vapor)
    long_up = 0.4 * (1.0 + 0.2 * surface_temp) ** 4
    heat_flux = (0.94 * short_down + long_down - long_up - sensible - latent) * sea_share
    surface = jnp.stack([surface_temp, sensible, latent, long_up]) * sea_share[None]
    return (stress_x, stress_y, heat_flux, surface)

def reference(atm_flux, send_block, send_count, recv_block, recv_weight, sea_temp, ocean_mask):
    group_count = N_GRP
    tile_count = N_TILE
    device_count = group_count * tile_count
    slot_range = jnp.arange(CAP, dtype=jnp.int32)
    blocks = atm_flux.reshape(NF, device_count, ABLK_DEV, BLK)

    def pick_slots(dev_blocks, send_index, pair_count):
        chosen = jnp.take(dev_blocks, send_index, axis=1)
        live_slots = (slot_range[None, :] < pair_count[:, None]).astype(jnp.float32)
        return chosen * live_slots[None, :, :, None]
    picked = jax.vmap(pick_slots, in_axes=(1, 0, 0))(blocks, send_block, send_count)
    picked = picked.reshape(group_count, tile_count, NF, tile_count, CAP, BLK)
    arrived = jnp.transpose(picked, (0, 3, 1, 4, 2, 5)).reshape(device_count, tile_count, CAP, NF, BLK)

    def remap_in(entries):
        weight, dest_block, incoming = entries
        weight_wide = weight.astype(jnp.float32)
        remapped = jnp.einsum('scij,scfj->scfi', weight_wide, incoming, precision=precise)
        onehot = (jnp.arange(OBLK, dtype=jnp.int32)[:, None] == dest_block.reshape(-1)[None, :]).astype(jnp.float32)
        landed = jnp.dot(onehot, remapped.reshape(tile_count * CAP, NF * BLK), precision=precise)
        return landed.reshape(OBLK, NF, BLK)
    landed = lax.map(remap_in, (recv_weight, recv_block, arrived))
    grid = landed.reshape(group_count, tile_count, OBLK, NF, BLK).transpose(3, 0, 1, 2, 4)
    grid = grid.reshape(NF, group_count, tile_count, OROW, OCOL).transpose(0, 1, 3, 2, 4).reshape(NF, NYO, NXO)
    stress_x, stress_y, heat_flux, surface = bulk_formula(grid, sea_temp, ocean_mask)
    sea_share = ocean_mask.astype(jnp.float32)
    fold_values = -jnp.flip(stress_x[NYO - 1])
    column_x = jnp.concatenate([jnp.zeros((1, NXO), jnp.float32), stress_x, fold_values[None]], axis=0)
    stress_curl = 0.5 * (jnp.roll(stress_y, -1, axis=1) - jnp.roll(stress_y, 1, axis=1)) - 0.5 * (column_x[2:] - column_x[:-2])
    stress_curl = stress_curl * sea_share
    per_device = surface.reshape(NB, group_count, OROW, tile_count, OCOL).transpose(1, 3, 0, 2, 4)
    per_device = per_device.reshape(device_count, NB, OBLK, BLK)

    def remap_out(entries):
        weight, dest_block, ocean_blocks = entries
        weight_wide = weight.astype(jnp.float32)
        chosen = jnp.take(ocean_blocks, dest_block, axis=1)
        return jnp.einsum('scij,fsci->scfj', weight_wide, chosen, precision=precise)
    returned = lax.map(remap_out, (recv_weight, recv_block, per_device))
    returned = returned.reshape(group_count, tile_count, tile_count, CAP, NB, BLK).transpose(0, 2, 1, 3, 4, 5)
    returned = returned.reshape(device_count, tile_count, CAP, NB, BLK)

    def gather_back(send_index, pair_count, pieces):
        live_slots = (slot_range[None, :] < pair_count[:, None]).astype(jnp.float32)
        pieces = pieces * live_slots[:, :, None, None]
        onehot = (jnp.arange(ABLK_DEV, dtype=jnp.int32)[:, None] == send_index.reshape(-1)[None, :]).astype(jnp.float32)
        total = jnp.dot(onehot, pieces.reshape(tile_count * CAP, NB * BLK), precision=precise)
        return total.reshape(ABLK_DEV, NB, BLK)
    atm_parts = jax.vmap(gather_back)(send_block, send_count, returned)
    atm_return = atm_parts.transpose(2, 0, 1, 3).reshape(NB, ACELLS)
    return (heat_flux, stress_curl, atm_return)
```

```python
import functools

import jax
import jax.numpy as jnp
from jax import lax
from jax.experimental import pallas as pl
from jax.experimental.pallas import tpu as pltpu
from jax.sharding import PartitionSpec as P

MESH = pl.DeviceIdType.MESH
f32, bf16 = jnp.float32, jnp.bfloat16


def split(x):
    hi = x.astype(bf16).astype(f32)
    return hi, x - hi


def iota(shape, dim):
    return lax.broadcasted_iota(jnp.int32, shape, dim)


def kernel(dims, atm, sblk, scnt, rblk, wgt, temp, mask, heat, curl, ret_out,
           atm_v, sblk_s, scnt_s, rblk_s, w_v, temp_v, mask_v, send_v, recv_v, rhs_v, surf_v,
           back_v, ret_v, rim_s, rim_r, heat_v, curl_v, out_v,
           in_sem, send_sem, recv_sem, bsend_sem, brecv_sem, hsend_sem, hrecv_sem, out_sem):
    G, T, NF, NB, C, B, A, R, H = dims
    nk = T * C
    g = lax.axis_index("grp")
    t = lax.axis_index("tile")
    pow2 = T & (T - 1) == 0
    target = (lambda d: t ^ d) if pow2 else (lambda d: lax.rem(t + d, T))
    source = (lambda d: t ^ d) if pow2 else (lambda d: lax.rem(t + T - d, T))

    bar = pltpu.get_barrier_semaphore()
    for d in range(1, T):
        pl.semaphore_signal(bar, inc=1, device_id=(g, target(d)), device_id_type=MESH)

    @pl.when(g > 0)
    def _():
        pl.semaphore_signal(bar, inc=1, device_id=(g - 1, t), device_id_type=MESH)

    @pl.when(g < G - 1)
    def _():
        pl.semaphore_signal(bar, inc=1, device_id=(g + 1, t), device_id_type=MESH)

    loads = [
        pltpu.make_async_copy(src, dst, in_sem.at[k])
        for k, (src, dst) in enumerate(
            [(sblk, sblk_s), (scnt, scnt_s), (atm, atm_v), (rblk, rblk_s), (temp, temp_v), (mask, mask_v), (wgt, w_v)]
        )
    ]
    for load in loads:
        load.start()
    for load in loads[:3]:
        load.wait()

    flux = [atm_v[:, b * B : (b + 1) * B] for b in range(A)]
    wanted = {}
    for d in range(T):
        u = target(d)
        count = scnt_s[0, u]
        for c in range(C):
            live = jnp.clip(count - c, 0, 1)
            wanted[d, c] = (sblk_s[0, u, c] + 1) * live - 1
            home = jnp.full((NF, B), wanted[d, c], jnp.int32)
            block = jnp.zeros((NF, B), f32)
            for b in range(A):
                block = jnp.where(home == b, flux[b], block)
            for f in range(NF):
                send_v[d, f * C + c : f * C + c + 1, :] = block[f : f + 1]

    pl.semaphore_wait(bar, T - 1 + (g > 0).astype(jnp.int32) + (g < G - 1).astype(jnp.int32))
    outgoing = {}
    for d in range(T - 1, 0, -1):
        outgoing[d] = pltpu.make_async_remote_copy(
            send_v.at[d], recv_v.at[d], send_sem.at[d], recv_sem.at[d],
            device_id=(g, target(d)), device_id_type=MESH)
        outgoing[d].start()

    for load in loads[3:6]:
        load.wait()
    halves = lambda ref: jnp.concatenate([ref[:, h * B : (h + 1) * B] for h in range(H)], axis=0)
    sea = halves(temp_v)
    share = halves(mask_v).astype(f32)
    vapor = jnp.exp(0.3 * sea)
    base = 1.0 + 0.2 * sea
    base = base * base
    long_up = 0.4 * (base * base)
    lane = iota((8, 2 * nk), 1)
    place = jnp.full((8, 2 * nk), -1, jnp.int32)
    spots = {}
    for d in range(T):
        for c in range(C):
            o = rblk_s[0, source(d), c]
            spots[d, c] = o
            k = d * C + c
            place = jnp.where((lane == k) | (lane == nk + k), o, place)
    where_row = iota((H * R, 2 * nk), 0)
    where_row = (where_row % R) * H + where_row // R
    onehot = (where_row == place[0:1]).astype(f32).astype(bf16)
    row8 = iota((8, B), 0)
    homes = []
    for d in range(T):
        for c in range(0, C, 2):
            homes.append(jnp.where(row8 < NB, wanted[d, c], wanted[d, c + 1]))
    loads[6].wait()

    rowf = iota((NF * C, B), 0) % C
    for d in range(T):
        if d:
            outgoing[d].wait_recv()
        held = send_v[0] if d == 0 else recv_v[d]
        hi, lo = split(held)
        lhs = jnp.concatenate([hi, lo], axis=0).astype(bf16)
        weight = w_v[0, source(d)].reshape(C * B, B)
        prod = lax.dot_general(lhs, weight, (((1,), (1,)), ((), ())), preferred_element_type=f32)
        prod = prod[: NF * C] + prod[NF * C :]
        mine = prod[:, :B]
        for c in range(1, C):
            mine = jnp.where(rowf == c, prod[:, c * B : (c + 1) * B], mine)
        for f in range(NF):
            rhs_v[d * C : (d + 1) * C, f * B : (f + 1) * B] = mine[f * C : (f + 1) * C]

    hi, lo = split(rhs_v[...])
    landed = jnp.dot(onehot, jnp.concatenate([hi, lo], axis=0).astype(bf16), preferred_element_type=f32)
    wind_u, wind_v, air_temp, air_vapor, short_down, long_down = [landed[:, f * B : (f + 1) * B] for f in range(NF)]
    speed = jnp.sqrt(wind_u * wind_u + wind_v * wind_v + 0.5)
    stress_x = 0.8 * speed * wind_u * share
    stress_y = 0.8 * speed * wind_v * share

    for h in range(H):
        rim_s[0, h : h + 1, :] = stress_x[(h + 1) * R - 1 : (h + 1) * R]
        rim_s[1, h : h + 1, :] = stress_x[h * R : h * R + 1]
    diag = iota((R, B), 0) == iota((R, B), 1)
    west_edge = stress_y[:R, 0:1]
    east_edge = stress_y[(H - 1) * R :, B - 1 : B]
    rim_s[2, 0:1, :] = jnp.sum(jnp.where(diag, east_edge, 0.0), axis=0, keepdims=True)
    rim_s[3, 0:1, :] = jnp.sum(jnp.where(diag, west_edge, 0.0), axis=0, keepdims=True)
    top = g == G - 1
    north_slot = jnp.where(top, 1, 0)
    north = pltpu.make_async_remote_copy(
        rim_s.at[0], rim_r.at[north_slot], hsend_sem.at[0], hrecv_sem.at[north_slot],
        device_id=(jnp.where(top, g, g + 1), jnp.where(top, T - 1 - t, t)), device_id_type=MESH)
    south = pltpu.make_async_remote_copy(
        rim_s.at[1], rim_r.at[1], hsend_sem.at[1], hrecv_sem.at[1],
        device_id=(jnp.maximum(g - 1, 0), t), device_id_type=MESH)
    east = pltpu.make_async_remote_copy(
        rim_s.at[2, pl.ds(0, 1)], rim_r.at[2, pl.ds(0, 1)], hsend_sem.at[2], hrecv_sem.at[2],
        device_id=(g, lax.rem(t + 1, T)), device_id_type=MESH)
    west = pltpu.make_async_remote_copy(
        rim_s.at[3, pl.ds(0, 1)], rim_r.at[3, pl.ds(0, 1)], hsend_sem.at[3], hrecv_sem.at[3],
        device_id=(g, lax.rem(t + T - 1, T)), device_id_type=MESH)
    north.start()
    pl.when(g > 0)(south.start)
    east.start()
    west.start()

    sensible = 0.6 * speed * (sea - air_temp)
    latent = 0.7 * speed * (vapor - air_vapor)
    for f, field in enumerate((sea, sensible, latent, long_up)):
        hi, lo = split(field * share)
        for h in range(H):
            surf_v[pl.ds(h, R, stride=H), f, :] = hi[h * R : (h + 1) * R]
            surf_v[pl.ds(h, R, stride=H), NB + f, :] = lo[h * R : (h + 1) * R]

    returns = {}
    zero = jnp.zeros((8, B), f32)
    for d in range(T - 1, -1, -1):
        rows = []
        for c in range(C):
            tile = surf_v[spots[d, c]]
            rows.append(jnp.concatenate([tile if k == c else zero for k in range(C)], axis=1))
        lhs = jnp.concatenate(rows, axis=0).astype(bf16)
        weight = w_v[0, source(d)].reshape(C * B, B)
        prod = jnp.dot(lhs, weight, preferred_element_type=f32)
        tiles = []
        for c in range(C):
            part = prod[c * 8 : (c + 1) * 8]
            tiles.append(part + pltpu.roll(part, NB, 0))
        for c in range(0, C, 2):
            back_v[d, c * NB : (c + 2) * NB, :] = jnp.where(row8 < NB, tiles[c], tiles[c + 1])
        if d:
            returns[d] = pltpu.make_async_remote_copy(
                back_v.at[d], ret_v.at[d], bsend_sem.at[d], brecv_sem.at[d],
                device_id=(g, source(d)), device_id_type=MESH)
            returns[d].start()

    heat_v[...] = jnp.concatenate(
        [((0.94 * short_down + long_down - long_up - sensible - latent) * share)[h * R : (h + 1) * R] for h in range(H)],
        axis=1)
    heat_copy = pltpu.make_async_copy(heat_v, heat, out_sem.at[0])
    heat_copy.start()

    north.wait_send()
    pl.when(g > 0)(south.wait_send)
    south_in = pltpu.make_async_remote_copy(
        rim_s.at[0], rim_r.at[0], hsend_sem.at[0], hrecv_sem.at[0],
        device_id=(jnp.maximum(g - 1, 0), t), device_id_type=MESH)
    pl.when(g > 0)(south_in.wait_recv)
    south.wait_recv()
    east.wait()
    west.wait()
    flip = (iota((B, B), 0) + iota((B, B), 1) == B - 1).astype(f32)
    north_rim = rim_r[1]
    mirrored = jnp.dot(north_rim, flip, precision=lax.Precision.HIGHEST, preferred_element_type=f32)
    row = iota((R, B), 0)
    col = iota((R, B), 1)
    west_col = jnp.sum(jnp.where(diag, rim_r[2, 0:1, :], 0.0), axis=1, keepdims=True)
    east_col = jnp.sum(jnp.where(diag, rim_r[3, 0:1, :], 0.0), axis=1, keepdims=True)
    sx = [stress_x[h * R : (h + 1) * R] for h in range(H)]
    sy = [stress_y[h * R : (h + 1) * R] for h in range(H)]
    ahead = [pltpu.roll(v, B - 1, 1) for v in sy]
    behind = [pltpu.roll(v, 1, 1) for v in sy]
    for h in range(H):
        nxt = ahead[h + 1] if h < H - 1 else east_col
        prv = behind[h - 1] if h else west_col
        dx = jnp.where(col == B - 1, nxt, ahead[h]) - jnp.where(col == 0, prv, behind[h])
        rim_n = jnp.where(top, -mirrored[H - 1 - h : H - h], north_rim[h : h + 1])
        rim_b = jnp.where(g == 0, 0.0, rim_r[0, h : h + 1, :])
        dy = jnp.where(row == R - 1, rim_n, pltpu.roll(sx[h], R - 1, 0)) - jnp.where(
            row == 0, rim_b, pltpu.roll(sx[h], 1, 0))
        curl_v[:, h * B : (h + 1) * B] = (0.5 * dx - 0.5 * dy) * share[h * R : (h + 1) * R]
    curl_copy = pltpu.make_async_copy(curl_v, curl, out_sem.at[1])
    curl_copy.start()

    totals = [zero] * A
    for d in range(T):
        if d:
            returns[d].wait_recv()
        for m in range(C // 2):
            piece = (ret_v if d else back_v)[d, m * 8 : (m + 1) * 8, :]
            home = homes[d * (C // 2) + m]
            for b in range(A):
                totals[b] = totals[b] + jnp.where(home == b, piece, 0.0)
    for b in range(A):
        out_v[:, b * B : (b + 1) * B] = (totals[b] + pltpu.roll(totals[b], NB, 0))[:NB]
    ret_copy = pltpu.make_async_copy(out_v, ret_out, out_sem.at[2])
    ret_copy.start()
    for d in range(1, T):
        outgoing[d].wait_send()
        returns[d].wait_send()
    heat_copy.wait()
    curl_copy.wait()
    ret_copy.wait()


def per_device(mesh, *args):
    atm, sblk, scnt, rblk, wgt, temp, mask = args
    G, T = mesh.shape["grp"], mesh.shape["tile"]
    NF, B, C, NB = atm.shape[0], wgt.shape[-1], sblk.shape[2], 4
    A = atm.shape[1] // B
    R, W = temp.shape
    H = W // B
    dims = (G, T, NF, NB, C, B, A, R, H)
    vm = pltpu.VMEM
    dma = pltpu.SemaphoreType.DMA
    return pl.pallas_call(
        functools.partial(kernel, dims),
        out_shape=(
            jax.ShapeDtypeStruct((R, W), f32),
            jax.ShapeDtypeStruct((R, W), f32),
            jax.ShapeDtypeStruct((NB, A * B), f32),
        ),
        in_specs=[pl.BlockSpec(memory_space=pl.ANY)] * 7,
        out_specs=[pl.BlockSpec(memory_space=pl.ANY)] * 3,
        scratch_shapes=[
            vm((NF, A * B), f32),
            pltpu.SMEM(sblk.shape, jnp.int32),
            pltpu.SMEM(scnt.shape, jnp.int32),
            pltpu.SMEM(rblk.shape, jnp.int32),
            vm(wgt.shape, wgt.dtype),
            vm((R, W), f32),
            vm((R, W), jnp.int32),
            vm((T, NF * C, B), f32),
            vm((T, NF * C, B), f32),
            vm((T * C, NF * B), f32),
            vm((H * R, 8, B), f32),
            vm((T, NB * C, B), f32),
            vm((T, NB * C, B), f32),
            vm((4, H, B), f32),
            vm((4, H, B), f32),
            vm((R, W), f32),
            vm((R, W), f32),
            vm((NB, A * B), f32),
            dma((7,)),
            dma((T,)),
            dma((T,)),
            dma((T,)),
            dma((T,)),
            dma((4,)),
            dma((4,)),
            dma((3,)),
        ],
        compiler_params=pltpu.CompilerParams(collective_id=0, has_side_effects=True),
        name="exchange",
    )(*args)


def solution(mesh):
    placed = (
        P(None, ("grp", "tile")),
        P(("grp", "tile"), None, None),
        P(("grp", "tile"), None),
        P(("grp", "tile"), None, None),
        P(("grp", "tile"), None, None, None, None),
        P("grp", "tile"),
        P("grp", "tile"),
    )
    return jax.shard_map(
        functools.partial(per_device, mesh),
        mesh=mesh,
        in_specs=placed,
        out_specs=(P("grp", "tile"), P("grp", "tile"), P(None, ("grp", "tile"))),
        check_vma=False,
    )
```

```python
import functools

import jax
import jax.numpy as jnp
from jax import lax
from jax.experimental import pallas as pl
from jax.experimental.pallas import tpu as pltpu
from jax.sharding import PartitionSpec as P

MESH = pl.DeviceIdType.MESH
f32, bf16 = jnp.float32, jnp.bfloat16


def split(x):
    hi = x.astype(bf16).astype(f32)
    return hi, x - hi


def iota(shape, dim):
    return lax.broadcasted_iota(jnp.int32, shape, dim)


def kernel(dims, atm, sblk, scnt, rblk, wgt, temp, mask, heat_v, curl_v, out_v,
           atm_v, sblk_s, scnt_s, rblk_s, w_v, temp_v, mask_v, send_v, recv_v, rhs_v, surf_v,
           back_v, ret_v, rim_s, rim_r,
           in_sem, send_sem, recv_sem, bsend_sem, brecv_sem, hsend_sem, hrecv_sem):
    G, T, NF, NB, C, B, A, R, H = dims
    nk = T * C
    g = lax.axis_index("grp")
    t = lax.axis_index("tile")
    pow2 = T & (T - 1) == 0
    target = (lambda d: t ^ d) if pow2 else (lambda d: lax.rem(t + d, T))
    source = (lambda d: t ^ d) if pow2 else (lambda d: lax.rem(t + T - d, T))

    bar = pltpu.get_barrier_semaphore()
    for d in range(1, T):
        pl.semaphore_signal(bar, inc=1, device_id=(g, target(d)), device_id_type=MESH)

    @pl.when(g > 0)
    def _():
        pl.semaphore_signal(bar, inc=1, device_id=(g - 1, t), device_id_type=MESH)

    @pl.when(g < G - 1)
    def _():
        pl.semaphore_signal(bar, inc=1, device_id=(g + 1, t), device_id_type=MESH)

    loads = [
        pltpu.make_async_copy(src, dst, in_sem.at[k])
        for k, (src, dst) in enumerate(
            [(sblk, sblk_s), (scnt, scnt_s), (atm, atm_v), (rblk, rblk_s), (temp, temp_v), (mask, mask_v), (wgt, w_v)]
        )
    ]
    for load in loads:
        load.start()
    for load in loads[:3]:
        load.wait()

    flux = [atm_v[:, b * B : (b + 1) * B] for b in range(A)]
    wanted = {}
    for d in range(T):
        u = target(d)
        count = scnt_s[0, u]
        for c in range(C):
            live = jnp.clip(count - c, 0, 1)
            wanted[d, c] = (sblk_s[0, u, c] + 1) * live - 1
            home = jnp.full((NF, B), wanted[d, c], jnp.int32)
            block = jnp.zeros((NF, B), f32)
            for b in range(A):
                block = jnp.where(home == b, flux[b], block)
            for f in range(NF):
                send_v[d, f * C + c : f * C + c + 1, :] = block[f : f + 1]

    pl.semaphore_wait(bar, T - 1 + (g > 0).astype(jnp.int32) + (g < G - 1).astype(jnp.int32))
    outgoing = {}
    for d in range(T - 1, 0, -1):
        outgoing[d] = pltpu.make_async_remote_copy(
            send_v.at[d], recv_v.at[d], send_sem.at[d], recv_sem.at[d],
            device_id=(g, target(d)), device_id_type=MESH)
        outgoing[d].start()

    for load in loads[3:6]:
        load.wait()
    halves = lambda ref: jnp.concatenate([ref[:, h * B : (h + 1) * B] for h in range(H)], axis=0)
    sea = halves(temp_v)
    share = halves(mask_v).astype(f32)
    vapor = jnp.exp(0.3 * sea)
    base = 1.0 + 0.2 * sea
    base = base * base
    long_up = 0.4 * (base * base)
    lane = iota((8, 2 * nk), 1)
    place = jnp.full((8, 2 * nk), -1, jnp.int32)
    spots = {}
    for d in range(T):
        for c in range(C):
            o = rblk_s[0, source(d), c]
            spots[d, c] = o
            k = d * C + c
            place = jnp.where((lane == k) | (lane == nk + k), o, place)
    where_row = iota((H * R, 2 * nk), 0)
    where_row = (where_row % R) * H + where_row // R
    onehot = (where_row == place[0:1]).astype(f32).astype(bf16)
    row8 = iota((8, B), 0)
    homes = []
    for d in range(T):
        for c in range(0, C, 2):
            homes.append(jnp.where(row8 < NB, wanted[d, c], wanted[d, c + 1]))
    loads[6].wait()

    rowf = iota((NF * C, B), 0) % C
    for d in range(T):
        if d:
            outgoing[d].wait_recv()
        held = send_v[0] if d == 0 else recv_v[d]
        hi, lo = split(held)
        lhs = jnp.concatenate([hi, lo], axis=0).astype(bf16)
        weight = w_v[0, source(d)].reshape(C * B, B)
        prod = lax.dot_general(lhs, weight, (((1,), (1,)), ((), ())), preferred_element_type=f32)
        prod = prod[: NF * C] + prod[NF * C :]
        mine = prod[:, :B]
        for c in range(1, C):
            mine = jnp.where(rowf == c, prod[:, c * B : (c + 1) * B], mine)
        for f in range(NF):
            rhs_v[d * C : (d + 1) * C, f * B : (f + 1) * B] = mine[f * C : (f + 1) * C]

    hi, lo = split(rhs_v[...])
    landed = jnp.dot(onehot, jnp.concatenate([hi, lo], axis=0).astype(bf16), preferred_element_type=f32)
    wind_u, wind_v, air_temp, air_vapor, short_down, long_down = [landed[:, f * B : (f + 1) * B] for f in range(NF)]
    speed = jnp.sqrt(wind_u * wind_u + wind_v * wind_v + 0.5)
    stress_x = 0.8 * speed * wind_u * share
    stress_y = 0.8 * speed * wind_v * share

    for h in range(H):
        rim_s[0, h : h + 1, :] = stress_x[(h + 1) * R - 1 : (h + 1) * R]
        rim_s[1, h : h + 1, :] = stress_x[h * R : h * R + 1]
    diag = iota((R, B), 0) == iota((R, B), 1)
    west_edge = stress_y[:R, 0:1]
    east_edge = stress_y[(H - 1) * R :, B - 1 : B]
    rim_s[2, 0:1, :] = jnp.sum(jnp.where(diag, east_edge, 0.0), axis=0, keepdims=True)
    rim_s[3, 0:1, :] = jnp.sum(jnp.where(diag, west_edge, 0.0), axis=0, keepdims=True)
    top = g == G - 1
    north_slot = jnp.where(top, 1, 0)
    north = pltpu.make_async_remote_copy(
        rim_s.at[0], rim_r.at[north_slot], hsend_sem.at[0], hrecv_sem.at[north_slot],
        device_id=(jnp.where(top, g, g + 1), jnp.where(top, T - 1 - t, t)), device_id_type=MESH)
    south = pltpu.make_async_remote_copy(
        rim_s.at[1], rim_r.at[1], hsend_sem.at[1], hrecv_sem.at[1],
        device_id=(jnp.maximum(g - 1, 0), t), device_id_type=MESH)
    east = pltpu.make_async_remote_copy(
        rim_s.at[2, pl.ds(0, 1)], rim_r.at[2, pl.ds(0, 1)], hsend_sem.at[2], hrecv_sem.at[2],
        device_id=(g, lax.rem(t + 1, T)), device_id_type=MESH)
    west = pltpu.make_async_remote_copy(
        rim_s.at[3, pl.ds(0, 1)], rim_r.at[3, pl.ds(0, 1)], hsend_sem.at[3], hrecv_sem.at[3],
        device_id=(g, lax.rem(t + T - 1, T)), device_id_type=MESH)
    north.start()
    pl.when(g > 0)(south.start)
    east.start()
    west.start()

    sensible = 0.6 * speed * (sea - air_temp)
    latent = 0.7 * speed * (vapor - air_vapor)
    for f, field in enumerate((sea, sensible, latent, long_up)):
        hi, lo = split(field * share)
        for h in range(H):
            surf_v[pl.ds(h, R, stride=H), f, :] = hi[h * R : (h + 1) * R]
            surf_v[pl.ds(h, R, stride=H), NB + f, :] = lo[h * R : (h + 1) * R]

    returns = {}
    zero = jnp.zeros((8, B), f32)
    for d in range(T - 1, -1, -1):
        rows = []
        for c in range(C):
            tile = surf_v[spots[d, c]]
            rows.append(jnp.concatenate([tile if k == c else zero for k in range(C)], axis=1))
        lhs = jnp.concatenate(rows, axis=0).astype(bf16)
        weight = w_v[0, source(d)].reshape(C * B, B)
        prod = jnp.dot(lhs, weight, preferred_element_type=f32)
        tiles = []
        for c in range(C):
            part = prod[c * 8 : (c + 1) * 8]
            tiles.append(part + pltpu.roll(part, NB, 0))
        for c in range(0, C, 2):
            back_v[d, c * NB : (c + 2) * NB, :] = jnp.where(row8 < NB, tiles[c], tiles[c + 1])
        if d:
            returns[d] = pltpu.make_async_remote_copy(
                back_v.at[d], ret_v.at[d], bsend_sem.at[d], brecv_sem.at[d],
                device_id=(g, source(d)), device_id_type=MESH)
            returns[d].start()

    heat_v[...] = jnp.concatenate(
        [((0.94 * short_down + long_down - long_up - sensible - latent) * share)[h * R : (h + 1) * R] for h in range(H)],
        axis=1)

    north.wait_send()
    pl.when(g > 0)(south.wait_send)
    south_in = pltpu.make_async_remote_copy(
        rim_s.at[0], rim_r.at[0], hsend_sem.at[0], hrecv_sem.at[0],
        device_id=(jnp.maximum(g - 1, 0), t), device_id_type=MESH)
    pl.when(g > 0)(south_in.wait_recv)
    south.wait_recv()
    east.wait()
    west.wait()
    flip = (iota((B, B), 0) + iota((B, B), 1) == B - 1).astype(f32)
    north_rim = rim_r[1]
    mirrored = jnp.dot(north_rim, flip, precision=lax.Precision.HIGHEST, preferred_element_type=f32)
    row = iota((R, B), 0)
    col = iota((R, B), 1)
    west_col = jnp.sum(jnp.where(diag, rim_r[2, 0:1, :], 0.0), axis=1, keepdims=True)
    east_col = jnp.sum(jnp.where(diag, rim_r[3, 0:1, :], 0.0), axis=1, keepdims=True)
    sx = [stress_x[h * R : (h + 1) * R] for h in range(H)]
    sy = [stress_y[h * R : (h + 1) * R] for h in range(H)]
    ahead = [pltpu.roll(v, B - 1, 1) for v in sy]
    behind = [pltpu.roll(v, 1, 1) for v in sy]
    for h in range(H):
        nxt = ahead[h + 1] if h < H - 1 else east_col
        prv = behind[h - 1] if h else west_col
        dx = jnp.where(col == B - 1, nxt, ahead[h]) - jnp.where(col == 0, prv, behind[h])
        rim_n = jnp.where(top, -mirrored[H - 1 - h : H - h], north_rim[h : h + 1])
        rim_b = jnp.where(g == 0, 0.0, rim_r[0, h : h + 1, :])
        dy = jnp.where(row == R - 1, rim_n, pltpu.roll(sx[h], R - 1, 0)) - jnp.where(
            row == 0, rim_b, pltpu.roll(sx[h], 1, 0))
        curl_v[:, h * B : (h + 1) * B] = (0.5 * dx - 0.5 * dy) * share[h * R : (h + 1) * R]

    totals = [zero] * A
    for d in range(T):
        if d:
            returns[d].wait_recv()
        for m in range(C // 2):
            piece = (ret_v if d else back_v)[d, m * 8 : (m + 1) * 8, :]
            home = homes[d * (C // 2) + m]
            for b in range(A):
                totals[b] = totals[b] + jnp.where(home == b, piece, 0.0)
    for b in range(A):
        out_v[:, b * B : (b + 1) * B] = (totals[b] + pltpu.roll(totals[b], NB, 0))[:NB]
    for d in range(1, T):
        outgoing[d].wait_send()
        returns[d].wait_send()


def put_out(a, b, c, x, y, z, sem):
    copies = [pltpu.make_async_copy(src, dst, sem.at[k]) for k, (src, dst) in enumerate(((a, x), (b, y), (c, z)))]
    for copy in copies:
        copy.start()
    for copy in copies:
        copy.wait()


def per_device(mesh, *args):
    atm, sblk, scnt, rblk, wgt, temp, mask = args
    G, T = mesh.shape["grp"], mesh.shape["tile"]
    NF, B, C, NB = atm.shape[0], wgt.shape[-1], sblk.shape[2], 4
    A = atm.shape[1] // B
    R, W = temp.shape
    H = W // B
    dims = (G, T, NF, NB, C, B, A, R, H)
    vm = pltpu.VMEM
    dma = pltpu.SemaphoreType.DMA
    held = pl.pallas_call(
        functools.partial(kernel, dims),
        out_shape=(vm((R, W), f32), vm((R, W), f32), vm((NB, A * B), f32)),
        in_specs=[pl.BlockSpec(memory_space=pl.ANY)] * 7,
        out_specs=[pl.BlockSpec(memory_space=vm)] * 3,
        scratch_shapes=[
            vm((NF, A * B), f32),
            pltpu.SMEM(sblk.shape, jnp.int32),
            pltpu.SMEM(scnt.shape, jnp.int32),
            pltpu.SMEM(rblk.shape, jnp.int32),
            vm(wgt.shape, wgt.dtype),
            vm((R, W), f32),
            vm((R, W), jnp.int32),
            vm((T, NF * C, B), f32),
            vm((T, NF * C, B), f32),
            vm((T * C, NF * B), f32),
            vm((H * R, 8, B), f32),
            vm((T, NB * C, B), f32),
            vm((T, NB * C, B), f32),
            vm((4, H, B), f32),
            vm((4, H, B), f32),
            dma((7,)),
            dma((T,)),
            dma((T,)),
            dma((T,)),
            dma((T,)),
            dma((4,)),
            dma((4,)),
        ],
        compiler_params=pltpu.CompilerParams(collective_id=0, has_side_effects=True),
        name="exchange",
    )(*args)
    return pl.pallas_call(
        put_out,
        out_shape=[jax.ShapeDtypeStruct(v.shape, v.dtype) for v in held],
        in_specs=[pl.BlockSpec(memory_space=vm)] * 3,
        out_specs=[pl.BlockSpec(memory_space=pl.ANY)] * 3,
        scratch_shapes=[dma((3,))],
        name="put_out",
    )(*[pltpu.with_memory_space_constraint(v, vm) for v in held])


def solution(mesh):
    placed = (
        P(None, ("grp", "tile")),
        P(("grp", "tile"), None, None),
        P(("grp", "tile"), None),
        P(("grp", "tile"), None, None),
        P(("grp", "tile"), None, None, None, None),
        P("grp", "tile"),
        P("grp", "tile"),
    )
    return jax.shard_map(
        functools.partial(per_device, mesh),
        mesh=mesh,
        in_specs=placed,
        out_specs=(P("grp", "tile"), P("grp", "tile"), P(None, ("grp", "tile"))),
        check_vma=False,
    )
```

```python
import functools

import jax
import jax.numpy as jnp
from jax import lax
from jax.experimental import pallas as pl
from jax.experimental.pallas import tpu as pltpu
from jax.sharding import PartitionSpec as P

MESH = pl.DeviceIdType.MESH
f32, bf16 = jnp.float32, jnp.bfloat16


def split(x):
    hi = x.astype(bf16).astype(f32)
    return hi, x - hi


def iota(shape, dim):
    return lax.broadcasted_iota(jnp.int32, shape, dim)


def kernel(dims, atm, sblk, scnt, rblk, wgt, temp, mask, heat_v, curl_v, out_v,
           atm_v, sblk_s, scnt_s, rblk_s, w_v, temp_v, mask_v, send_v, recv_v, back_v, ret_v, rim_s, rim_r,
           in_sem, send_sem, recv_sem, bsend_sem, brecv_sem, hsend_sem, hrecv_sem):
    G, T, NF, NB, C, B, A, R, H = dims
    nk = T * C
    g = lax.axis_index("grp")
    t = lax.axis_index("tile")
    pow2 = T & (T - 1) == 0
    target = (lambda d: t ^ d) if pow2 else (lambda d: lax.rem(t + d, T))
    source = (lambda d: t ^ d) if pow2 else (lambda d: lax.rem(t + T - d, T))

    bar = pltpu.get_barrier_semaphore()
    for d in range(1, T):
        pl.semaphore_signal(bar, inc=1, device_id=(g, target(d)), device_id_type=MESH)

    @pl.when(g > 0)
    def _():
        pl.semaphore_signal(bar, inc=1, device_id=(g - 1, t), device_id_type=MESH)

    @pl.when(g < G - 1)
    def _():
        pl.semaphore_signal(bar, inc=1, device_id=(g + 1, t), device_id_type=MESH)

    loads = [
        pltpu.make_async_copy(src, dst, in_sem.at[k])
        for k, (src, dst) in enumerate(
            [(sblk, sblk_s), (scnt, scnt_s), (atm, atm_v), (rblk, rblk_s), (temp, temp_v), (mask, mask_v), (wgt, w_v)]
        )
    ]
    for load in loads:
        load.start()
    for load in loads[:3]:
        load.wait()

    flux = [atm_v[:, b * B : (b + 1) * B] for b in range(A)]
    wanted = {}
    for d in range(T):
        u = target(d)
        count = scnt_s[0, u]
        for c in range(C):
            live = jnp.clip(count - c, 0, 1)
            wanted[d, c] = (sblk_s[0, u, c] + 1) * live - 1
            home = jnp.full((NF, B), wanted[d, c], jnp.int32)
            block = jnp.zeros((NF, B), f32)
            for b in range(A):
                block = jnp.where(home == b, flux[b], block)
            for f in range(NF):
                send_v[d, f * C + c : f * C + c + 1, :] = block[f : f + 1]

    pl.semaphore_wait(bar, T - 1 + (g > 0).astype(jnp.int32) + (g < G - 1).astype(jnp.int32))
    outgoing = {}
    for d in range(T - 1, 0, -1):
        outgoing[d] = pltpu.make_async_remote_copy(
            send_v.at[d], recv_v.at[d], send_sem.at[0], recv_sem.at[d - 1],
            device_id=(g, target(d)), device_id_type=MESH)
        outgoing[d].start()

    for load in loads[3:6]:
        load.wait()
    halves = lambda ref: jnp.concatenate([ref[:, h * B : (h + 1) * B] for h in range(H)], axis=0)
    sea = halves(temp_v)
    share = halves(mask_v).astype(f32)
    vapor = jnp.exp(0.3 * sea)
    base = 1.0 + 0.2 * sea
    base = base * base
    long_up = 0.4 * (base * base)
    per = 2 * C
    cells = H * R
    order = lambda o: (o % R) * H + o // R
    lane = iota((8, 2 * T * per), 1)
    row8 = iota((8, B), 0)
    place = jnp.full((8, 2 * T * per), -1, jnp.int32)
    picks, homes = [], []
    col = iota((per, 2 * cells), 1)
    prow = iota((per, 2 * cells), 0)
    for d in range(T):
        pick = jnp.full((per, 2 * cells), -1, jnp.int32)
        home = jnp.full((8, B), -1, jnp.int32)
        for c in range(C):
            o = rblk_s[0, source(d), c]
            place = jnp.where((lane // per % T == d) & (lane % C == c), o, place)
            pick = jnp.where(prow % C == c, o, pick)
            home = jnp.where(row8 % C == c, wanted[d, c], home)
        picks.append(jnp.where((order(col % cells) == pick) & (col // cells == prow // C), 1.0, 0.0))
        homes.append(home)
    gather = jnp.concatenate(picks, axis=0).astype(bf16)
    land_row = iota((2 * cells, 2 * T * per), 0)
    land_col = iota((2 * cells, 2 * T * per), 1)
    onehot = jnp.where(
        (order(land_row % cells) == place[0:1]) & (land_row // cells == land_col % per // C), 1.0, 0.0).astype(bf16)
    loads[6].wait()

    rowf = iota((NF * C, B), 0) % C
    parts = []
    for d in range(T):
        if d:
            outgoing[d].wait_recv()
        held = send_v[0] if d == 0 else recv_v[d]
        hi, lo = split(held)
        lhs = jnp.concatenate([hi, lo], axis=0).astype(bf16)
        weight = w_v[0, source(d)].reshape(C * B, B)
        prod = lax.dot_general(lhs, weight, (((1,), (1,)), ((), ())), preferred_element_type=f32)
        prod = prod[: NF * C] + prod[NF * C :]
        mine = prod[:, :B]
        for c in range(1, C):
            mine = jnp.where(rowf == c, prod[:, c * B : (c + 1) * B], mine)
        parts.append(jnp.concatenate([mine[k * per : (k + 1) * per] for k in range(NF // 2)], axis=1))

    hi, lo = split(jnp.concatenate(parts, axis=0))
    landed = jnp.dot(onehot, jnp.concatenate([hi, lo], axis=0).astype(bf16), preferred_element_type=f32)
    wind_u, wind_v, air_temp, air_vapor, short_down, long_down = [
        landed[f % 2 * cells : (f % 2 + 1) * cells, f // 2 * B : (f // 2 + 1) * B] for f in range(NF)]
    speed = jnp.sqrt(wind_u * wind_u + wind_v * wind_v + 0.5)
    stress_x = 0.8 * speed * wind_u * share
    stress_y = 0.8 * speed * wind_v * share

    for h in range(H):
        rim_s[0, h : h + 1, :] = stress_x[(h + 1) * R - 1 : (h + 1) * R]
        rim_s[1, h : h + 1, :] = stress_x[h * R : h * R + 1]
    diag = iota((R, B), 0) == iota((R, B), 1)
    west_edge = stress_y[:R, 0:1]
    east_edge = stress_y[(H - 1) * R :, B - 1 : B]
    rim_s[2, 0:1, :] = jnp.sum(jnp.where(diag, east_edge, 0.0), axis=0, keepdims=True)
    rim_s[3, 0:1, :] = jnp.sum(jnp.where(diag, west_edge, 0.0), axis=0, keepdims=True)
    top = g == G - 1
    north_slot = jnp.where(top, 1, 0)
    north = pltpu.make_async_remote_copy(
        rim_s.at[0], rim_r.at[north_slot], hsend_sem.at[0], hrecv_sem.at[north_slot],
        device_id=(jnp.where(top, g, g + 1), jnp.where(top, T - 1 - t, t)), device_id_type=MESH)
    south = pltpu.make_async_remote_copy(
        rim_s.at[1], rim_r.at[1], hsend_sem.at[1], hrecv_sem.at[1],
        device_id=(jnp.maximum(g - 1, 0), t), device_id_type=MESH)
    east = pltpu.make_async_remote_copy(
        rim_s.at[2, pl.ds(0, 1)], rim_r.at[2, pl.ds(0, 1)], hsend_sem.at[2], hrecv_sem.at[2],
        device_id=(g, lax.rem(t + 1, T)), device_id_type=MESH)
    west = pltpu.make_async_remote_copy(
        rim_s.at[3, pl.ds(0, 1)], rim_r.at[3, pl.ds(0, 1)], hsend_sem.at[3], hrecv_sem.at[3],
        device_id=(g, lax.rem(t + T - 1, T)), device_id_type=MESH)
    north.start()
    pl.when(g > 0)(south.start)
    east.start()
    west.start()

    sensible = 0.6 * speed * (sea - air_temp)
    latent = 0.7 * speed * (vapor - air_vapor)
    pieces = [split(field * share) for field in (sea, sensible, latent, long_up)]
    surface = jnp.concatenate(
        [jnp.concatenate([pieces[2 * k + e][p] for p in range(2) for k in range(NB // 2)], axis=1) for e in range(2)],
        axis=0).astype(bf16)
    chosen = jnp.dot(gather, surface, preferred_element_type=f32)

    returns = {}
    zero = jnp.zeros((8, B), f32)
    rowb = iota((2 * NB * C, B), 0) % C
    for d in range(T - 1, -1, -1):
        tile = chosen[d * per : (d + 1) * per]
        tile = jnp.concatenate([tile[:, k * B : (k + 1) * B] for k in range(NB)], axis=0)
        lhs = jnp.concatenate([jnp.where(rowb == c, tile, 0.0) for c in range(C)], axis=1).astype(bf16)
        weight = w_v[0, source(d)].reshape(C * B, B)
        prod = jnp.dot(lhs, weight, preferred_element_type=f32)
        back_v[d] = prod[: NB * C] + prod[NB * C :]
        if d:
            returns[d] = pltpu.make_async_remote_copy(
                back_v.at[d], ret_v.at[d], bsend_sem.at[0], brecv_sem.at[0],
                device_id=(g, source(d)), device_id_type=MESH)
            returns[d].start()

    heat_v[...] = jnp.concatenate(
        [((0.94 * short_down + long_down - long_up - sensible - latent) * share)[h * R : (h + 1) * R] for h in range(H)],
        axis=1)

    north.wait_send()
    pl.when(g > 0)(south.wait_send)
    south_in = pltpu.make_async_remote_copy(
        rim_s.at[0], rim_r.at[0], hsend_sem.at[0], hrecv_sem.at[0],
        device_id=(jnp.maximum(g - 1, 0), t), device_id_type=MESH)
    pl.when(g > 0)(south_in.wait_recv)
    south.wait_recv()
    east.wait()
    west.wait()
    flip = (iota((B, B), 0) + iota((B, B), 1) == B - 1).astype(f32)
    north_rim = rim_r[1]
    mirrored = jnp.dot(north_rim, flip, precision=lax.Precision.HIGHEST, preferred_element_type=f32)
    row = iota((R, B), 0)
    col = iota((R, B), 1)
    west_col = jnp.sum(jnp.where(diag, rim_r[2, 0:1, :], 0.0), axis=1, keepdims=True)
    east_col = jnp.sum(jnp.where(diag, rim_r[3, 0:1, :], 0.0), axis=1, keepdims=True)
    sx = [stress_x[h * R : (h + 1) * R] for h in range(H)]
    sy = [stress_y[h * R : (h + 1) * R] for h in range(H)]
    ahead = [pltpu.roll(v, B - 1, 1) for v in sy]
    behind = [pltpu.roll(v, 1, 1) for v in sy]
    for h in range(H):
        nxt = ahead[h + 1] if h < H - 1 else east_col
        prv = behind[h - 1] if h else west_col
        dx = jnp.where(col == B - 1, nxt, ahead[h]) - jnp.where(col == 0, prv, behind[h])
        rim_n = jnp.where(top, -mirrored[H - 1 - h : H - h], north_rim[h : h + 1])
        rim_b = jnp.where(g == 0, 0.0, rim_r[0, h : h + 1, :])
        dy = jnp.where(row == R - 1, rim_n, pltpu.roll(sx[h], R - 1, 0)) - jnp.where(
            row == 0, rim_b, pltpu.roll(sx[h], 1, 0))
        curl_v[:, h * B : (h + 1) * B] = (0.5 * dx - 0.5 * dy) * share[h * R : (h + 1) * R]

    others = pl.ds(1, T - 1)
    whole = lambda ref, sem: pltpu.make_async_copy(ref.at[others], ref.at[others], sem.at[0])
    totals = {(b, k): zero for b in range(A) for k in range(NB // 2)}
    for d in range(T):
        if d == 1:
            whole(ret_v, brecv_sem).wait()
        for k in range(NB // 2):
            piece = (ret_v if d else back_v)[d, k * per : (k + 1) * per, :]
            for b in range(A):
                totals[b, k] = totals[b, k] + jnp.where(homes[d] == b, piece, 0.0)
    for b in range(A):
        for k in range(NB // 2):
            v = totals[b, k].reshape(2, C, B).sum(axis=1)
            out_v[2 * k : 2 * k + 2, b * B : (b + 1) * B] = v
    whole(send_v, send_sem).wait()
    whole(back_v, bsend_sem).wait()


def put_out(a, b, c, x, y, z, sem):
    copies = [pltpu.make_async_copy(src, dst, sem.at[k]) for k, (src, dst) in enumerate(((a, x), (b, y), (c, z)))]
    for copy in copies:
        copy.start()
    for copy in copies:
        copy.wait()


def per_device(mesh, *args):
    atm, sblk, scnt, rblk, wgt, temp, mask = args
    G, T = mesh.shape["grp"], mesh.shape["tile"]
    NF, B, C, NB = atm.shape[0], wgt.shape[-1], sblk.shape[2], 4
    A = atm.shape[1] // B
    R, W = temp.shape
    H = W // B
    dims = (G, T, NF, NB, C, B, A, R, H)
    vm = pltpu.VMEM
    dma = pltpu.SemaphoreType.DMA
    held = pl.pallas_call(
        functools.partial(kernel, dims),
        out_shape=(vm((R, W), f32), vm((R, W), f32), vm((NB, A * B), f32)),
        in_specs=[pl.BlockSpec(memory_space=pl.ANY)] * 7,
        out_specs=[pl.BlockSpec(memory_space=vm)] * 3,
        scratch_shapes=[
            vm((NF, A * B), f32),
            pltpu.SMEM(sblk.shape, jnp.int32),
            pltpu.SMEM(scnt.shape, jnp.int32),
            pltpu.SMEM(rblk.shape, jnp.int32),
            vm(wgt.shape, wgt.dtype),
            vm((R, W), f32),
            vm((R, W), jnp.int32),
            vm((T, NF * C, B), f32),
            vm((T, NF * C, B), f32),
            vm((T, NB * C, B), f32),
            vm((T, NB * C, B), f32),
            vm((4, H, B), f32),
            vm((4, H, B), f32),
            dma((7,)),
            dma((1,)),
            dma((T - 1,)),
            dma((1,)),
            dma((1,)),
            dma((4,)),
            dma((4,)),
        ],
        compiler_params=pltpu.CompilerParams(collective_id=0, has_side_effects=True),
        name="exchange",
    )(*args)
    return pl.pallas_call(
        put_out,
        out_shape=[jax.ShapeDtypeStruct(v.shape, v.dtype) for v in held],
        in_specs=[pl.BlockSpec(memory_space=vm)] * 3,
        out_specs=[pl.BlockSpec(memory_space=pl.ANY)] * 3,
        scratch_shapes=[dma((3,))],
        name="put_out",
    )(*[pltpu.with_memory_space_constraint(v, vm) for v in held])


def solution(mesh):
    placed = (
        P(None, ("grp", "tile")),
        P(("grp", "tile"), None, None),
        P(("grp", "tile"), None),
        P(("grp", "tile"), None, None),
        P(("grp", "tile"), None, None, None, None),
        P("grp", "tile"),
        P("grp", "tile"),
    )
    return jax.shard_map(
        functools.partial(per_device, mesh),
        mesh=mesh,
        in_specs=placed,
        out_specs=(P("grp", "tile"), P("grp", "tile"), P(None, ("grp", "tile"))),
        check_vma=False,
    )
```
